32 devices in a mesh: pos: 8 (over z, y), head: 4 (over x, core).
Axes of the slice: x: 2, y: 2, z: 4, core: 2. Of those that a mesh axis runs over, the one named last changes fastest.
Arguments:
- queries: bfloat16 [32, 512, 768], P('head', 'pos'), may hold values from -102 to 102
- latents: bfloat16 [32, 256, 1280], P('head', 'pos'), may hold values from -6 to 6
- w_query: bfloat16 [768, 768], replicated, may hold values from -0.21875 to 0.21875
- kv_gain: float32 [1280], replicated, may hold values from 0.1 to 1.9
- w_kv: bfloat16 [1280, 1536], replicated, may hold values from -0.15625 to 0.15625
- w_out: bfloat16 [768, 768], replicated, may hold values from -0.21875 to 0.21875
- mlp_gain: float32 [768], replicated, may hold values from 0.1 to 1.9
- w_up: bfloat16 [768, 768], replicated, may hold values from -0.21875 to 0.21875
- w_down: bfloat16 [768, 768], replicated, may hold values from -0.21875 to 0.21875
- w_vocab: bfloat16 [768, 262], replicated, may hold values from -0.59765625 to 0.59765625
- vocab_bias: float32 [262], replicated, may hold values from -4 to 4
- targets: int32 [32, 512], P('head', 'pos'), may hold values from 0 to 261
- mask: int32 [32, 512], P('head', 'pos'), may hold values from 0 to 1, as said below
Outputs:
- logits: bfloat16 [32, 512, 262], P('head', 'pos')
- loss: float32 [], replicated
The draws below stay inside these ranges and needn't reach their ends.
Inputs may be any that keep to these rules, and one draw needn't show every extreme that they name: `mask`: every sequence has at least one masked position.
All inputs are finite; a program needn't handle non-finite values.
Results may differ from the reference program's by a relative error of at most 0.0085.
Values may be sent and summed in bfloat16 or wider, within the bound.
A program may use at most 64 MiB of HBM per device.

```python
import jax
import jax.numpy as jnp
from jax import lax

D_MODEL = 768
D_LATENT = 1280
LATENTS = 256
VOCAB = 262
HEADS = 8
MLP_WIDTH = 768
BATCH = 32
SEQ = 512


def draw_queries(key, part):
    first_key = jax.random.fold_in(jax.random.fold_in(key, 11), 0)
    base = jax.random.normal(first_key, (BATCH, SEQ, D_MODEL), jnp.float32)
    return jnp.clip(base, -6.0, 6.0).astype(jnp.bfloat16)


def draw_mask(key, part):
    places = jnp.arange(SEQ, dtype=jnp.int32)
    ticket = jax.random.randint(jax.random.fold_in(key, 23), (BATCH, SEQ), 0, 1000)
    forced = jax.random.randint(jax.random.fold_in(key, 29), (BATCH, 1), 0, SEQ)
    drawn = ticket < 100 + 300 * places[None, :] // SEQ
    return jnp.logical_or(drawn, places[None, :] == forced).astype(jnp.int32)


def set_ends(array, key, smallest, largest):
    dims = array.shape
    index_at = [jax.random.randint(jax.random.fold_in(key, axis), (), 0, dims[axis]) for axis in range(len(dims))]
    array = array.at[tuple(index_at)].set(smallest)
    longest = dims.index(max(dims))
    index_at[longest] = (index_at[longest] + 1) % dims[longest]
    return array.at[tuple(index_at)].set(largest)


def shard_levels(stream_key, shape, cuts, smallest, largest):
    def one(position, blocks):
        draws = jax.random.uniform(jax.random.fold_in(jax.random.fold_in(stream_key, 6), position), (blocks,), jnp.float32, smallest / len(cuts), largest / len(cuts))
        return jnp.repeat(jnp.exp(draws), shape[position] // blocks).reshape((-1,) + (1,) * (len(shape) - position - 1))

    loudness = one(*cuts[0])
    for cut in cuts[1:]:
        loudness = loudness * one(*cut)
    return loudness


def noise(own_key, extent, deviation, most, pieces=(), kind=jnp.bfloat16):
    values = jax.random.normal(own_key, extent, jnp.float32) * deviation
    if len(pieces) > 0:
        values = shard_levels(own_key, extent, pieces, -0.22, 0.18) * values
    return jnp.clip(values, min=-most, max=most).astype(kind)


def setup_inputs(seed: int = 0) -> dict:
    keys = jax.random.split(jax.random.key(seed), 14)
    return {
        "queries": draw_queries(jax.random.fold_in(keys[13], 71), 0),
        "latents": noise(keys[1], (BATCH, LATENTS, D_LATENT), 1.0, 6.0, ((0, 4), (1, 8))),
        "w_query": noise(keys[2], (D_MODEL, D_MODEL), D_MODEL ** -0.5, 0.21875),
        "kv_gain": jnp.clip(1.0 + 0.18 * jax.random.normal(keys[3], (D_LATENT,), jnp.float32), 0.1, 1.9),
        "w_kv": noise(keys[4], (D_LATENT, 2 * D_MODEL), D_LATENT ** -0.5, 0.15625),
        "w_out": noise(keys[5], (D_MODEL, D_MODEL), D_MODEL ** -0.5, 0.21875),
        "mlp_gain": jnp.clip(1.0 + 0.18 * jax.random.normal(keys[6], (D_MODEL,), jnp.float32), 0.1, 1.9),
        "w_up": noise(keys[7], (D_MODEL, MLP_WIDTH), D_MODEL ** -0.5, 0.21875),
        "w_down": noise(keys[8], (MLP_WIDTH, D_MODEL), MLP_WIDTH ** -0.5, 0.21875),
        "w_vocab": noise(keys[9], (D_MODEL, VOCAB), 0.1, 0.59765625),
        "vocab_bias": noise(keys[10], (VOCAB,), 1.0, 4.0, (), jnp.float32),
        "targets": set_ends(jax.random.randint(keys[11], (BATCH, SEQ), 0, VOCAB), jax.random.fold_in(keys[11], 1), 0, VOCAB - 1).astype(jnp.int32),
        "mask": draw_mask(jax.random.fold_in(keys[13], 71), 0),
    }


epsilon = 1e-05

def layer_norm(field, gain):
    centre = field - lax.optimization_barrier(jnp.mean(field, axis=-1, keepdims=True))
    spread = lax.optimization_barrier(jnp.mean(centre * centre, axis=-1, keepdims=True))
    return centre * lax.rsqrt(spread + epsilon) * gain.astype(jnp.float32)

def reference(queries, latents, w_query, kv_gain, w_kv, w_out, mlp_gain, w_up, w_down, w_vocab, vocab_bias, targets, mask):
    head_dim = D_MODEL // HEADS
    scale_factor = float(head_dim) ** (-0.5)

    def one_sequence(items):
        seq_queries, seq_latents, seq_targets, seq_mask = items
        query_proj = jnp.dot(seq_queries, w_query, preferred_element_type=jnp.float32).astype(jnp.bfloat16)
        normed_lat = layer_norm(seq_latents.astype(jnp.float32), kv_gain).astype(jnp.bfloat16)
        key_value = jnp.dot(normed_lat, w_kv, preferred_element_type=jnp.float32).astype(jnp.bfloat16)
        heads_q = query_proj.reshape(SEQ, HEADS, head_dim).astype(jnp.float32)
        heads_k = key_value[:, :D_MODEL].reshape(LATENTS, HEADS, head_dim).astype(jnp.float32)
        heads_v = key_value[:, D_MODEL:].reshape(LATENTS, HEADS, head_dim).astype(jnp.float32)
        scores = jnp.einsum('phd,lhd->hpl', heads_q, heads_k) * scale_factor
        attn_weights = jax.nn.softmax(scores, axis=-1).astype(jnp.bfloat16)
        attended = jnp.einsum('hpl,lhd->phd', attn_weights.astype(jnp.float32), heads_v)
        attended = attended.astype(jnp.bfloat16).reshape(SEQ, D_MODEL)
        first = seq_queries.astype(jnp.float32) + jnp.dot(attended, w_out, preferred_element_type=jnp.float32)
        normed = layer_norm(first, mlp_gain).astype(jnp.bfloat16)
        hidden = jax.nn.gelu(jnp.dot(normed, w_up, preferred_element_type=jnp.float32)).astype(jnp.bfloat16)
        output = (first + jnp.dot(hidden, w_down, preferred_element_type=jnp.float32)).astype(jnp.bfloat16)
        full_logits = jnp.dot(output, w_vocab, preferred_element_type=jnp.float32) + vocab_bias.astype(jnp.float32)
        vocab_ids = jnp.arange(VOCAB, dtype=jnp.int32)
        picked = lax.optimization_barrier(jnp.sum(jnp.where(vocab_ids[None, :] == seq_targets[:, None], full_logits, 0.0), axis=-1))
        cross = jax.nn.logsumexp(full_logits, axis=-1) - picked
        weight_mask = seq_mask.astype(jnp.float32)
        return (full_logits.astype(jnp.bfloat16), jnp.sum(cross * weight_mask), jnp.sum(weight_mask))
    logits, loss_parts, count_parts = lax.map(one_sequence, (queries, latents, targets, mask))
    loss = jnp.sum(loss_parts) / jnp.sum(count_parts)
    return (logits, loss)
```

```python
import functools

import jax
import jax.numpy as jnp
from jax import lax
from jax.experimental import pallas as pl
from jax.experimental.pallas import tpu as pltpu
from jax.sharding import PartitionSpec as P

HEADS = 8
LAT_SPLIT = 1
ROW_SPLIT = 1
epsilon = 1e-05
MESH = pl.DeviceIdType.MESH


def layer_norm(field, gain):
    centre = field - jnp.mean(field, axis=-1, keepdims=True)
    spread = jnp.mean(centre * centre, axis=-1, keepdims=True)
    return centre * lax.rsqrt(spread + epsilon) * gain


def dot(left, right):
    return jnp.dot(left, right, preferred_element_type=jnp.float32)


def dot_last(left, right):
    return lax.dot_general(
        left, right, (((1,), (1,)), ((), ())), preferred_element_type=jnp.float32
    )


def kernel(
    n_pos,
    n_head,
    group,
    seqs,
    queries,
    latents,
    w_query_hbm,
    kv_gain,
    w_kv_hbm,
    w_out_hbm,
    mlp_gain,
    w_up_hbm,
    w_down_hbm,
    w_vocab_hbm,
    vocab_bias,
    targets,
    mask,
    out,
    loss_out,
    lat_stage,
    q_stage,
    lat_buf,
    q_buf,
    t_buf,
    m_buf,
    w_query,
    w_kv,
    w_out,
    w_up,
    w_down,
    w_vocab,
    kv_buf,
    logit_buf,
    acc,
    part_src,
    part_all,
    lat_send,
    lat_recv,
    q_send,
    q_recv,
    t_send,
    t_recv,
    m_send,
    m_recv,
    out_send,
    out_recv,
    p_send,
    p_recv,
    w_sem,
    stage_sem,
    stage_sems,
):
    me = lax.axis_index("pos")
    my_head = lax.axis_index("head")
    mine = lax.rem(me, group)
    base = me - mine

    def pos_peer(k):
        return lax.rem(base + (k // group) * group, n_pos) + lax.rem(mine + k % group, group)

    def group_peer(k):
        return base + lax.rem(mine + k, group)

    def group_source(k):
        return base + lax.rem(mine + group - k, group)

    block = max(1, group // 2)
    n_rows = n_pos // block
    staged_entry = 2 < n_rows <= 4
    row = me // block
    spot = lax.rem(me, block)

    def near(peer):
        gap = peer // block - row
        return jnp.logical_and(gap >= -1, gap <= 1)

    def signal_near(semaphore):
        for k in range(1, block):
            pl.semaphore_signal(
                semaphore,
                inc=1,
                device_id={"pos": row * block + lax.rem(spot + k, block)},
                device_id_type=MESH,
            )
        for shift, inside in ((-1, row > 0), (1, row < n_rows - 1)):

            @pl.when(inside)
            def neighbours(shift=shift):
                for k in range(block):
                    pl.semaphore_signal(
                        semaphore,
                        inc=1,
                        device_id={"pos": (row + shift) * block + k},
                        device_id_type=MESH,
                    )

    barrier = pltpu.get_barrier_semaphore()
    for k in range(1, n_head):
        pl.semaphore_signal(
            barrier, inc=1, device_id={"head": lax.rem(my_head + k, n_head)}, device_id_type=MESH
        )
    if staged_entry:
        signal_near(barrier)
        ends = (row > 0).astype(jnp.int32) + (row < n_rows - 1).astype(jnp.int32)
        n_near = block - 1 + block * ends
    else:
        for k in range(1, n_pos):
            pl.semaphore_signal(
                barrier, inc=1, device_id={"pos": pos_peer(k)}, device_id_type=MESH
            )
        n_near = n_pos - 1

    staged = (
        pltpu.make_async_copy(latents, lat_stage, stage_sem.at[0]),
        pltpu.make_async_copy(queries, q_stage, stage_sem.at[1]),
    )
    for copy in staged:
        copy.start()
    local = []

    def start_local(src, dst, sem):
        copy = pltpu.make_async_copy(src, dst, sem)
        copy.start()
        local.append(copy)

    start_local(queries.at[pl.ds(mine * seqs, seqs)], q_buf.at[0], q_recv.at[0])
    start_local(targets, t_buf.at[0], t_recv.at[0])
    start_local(mask, m_buf.at[0], m_recv.at[0])
    def lat_copy(k, i):
        peer = pos_peer(k)
        return pltpu.make_async_remote_copy(
            src_ref=lat_stage.at[lax.rem(peer, group) * seqs + i],
            dst_ref=lat_buf.at[i, k],
            send_sem=lat_send.at[i, k],
            recv_sem=lat_recv.at[i, k],
            device_id={"pos": peer},
            device_id_type=MESH,
        )

    def lat_local(i):
        return pltpu.make_async_copy(
            latents.at[mine * seqs + i], lat_buf.at[i, 0], lat_recv.at[i, 0]
        )

    def group_copy(k, src, dst, send, recv):
        return pltpu.make_async_remote_copy(
            src_ref=src,
            dst_ref=dst,
            send_sem=send.at[k],
            recv_sem=recv.at[k],
            device_id={"pos": group_peer(k)},
            device_id_type=MESH,
        )

    def q_copy(k):
        peer = lax.rem(mine + k, group)
        return group_copy(k, q_stage.at[pl.ds(peer * seqs, seqs)], q_buf.at[k], q_send, q_recv)

    def t_copy(k):
        return group_copy(k, targets, t_buf.at[k], t_send, t_recv)

    def m_copy(k):
        return group_copy(k, mask, m_buf.at[k], m_send, m_recv)

    def out_copy(k, i):
        return pltpu.make_async_remote_copy(
            src_ref=logit_buf.at[i, k],
            dst_ref=out.at[mine * seqs + i],
            send_sem=out_send.at[i, k],
            recv_sem=out_recv.at[i, k],
            device_id={"pos": group_source(k)},
            device_id_type=MESH,
        )

    def out_local(i):
        return pltpu.make_async_copy(
            logit_buf.at[i, 0], out.at[mine * seqs + i], out_recv.at[i, 0]
        )

    for i in range(seqs):
        lat_local(i).start()

    pl.semaphore_wait(barrier, n_near + n_head - 1)
    for copy in staged:
        copy.wait()

    cross = tuple(range(group, n_pos))
    inner = tuple(range(1, group))
    if staged_entry:
        for k in cross + inner:

            @pl.when(near(pos_peer(k)))
            def first(k=k):
                lat_copy(k, 0).start()

        for stage in range(n_rows - 2):
            signal_near(stage_sems.at[stage])
            pl.semaphore_wait(stage_sems.at[stage], n_near)
        for k in cross + inner:

            @pl.when(jnp.logical_not(near(pos_peer(k))))
            def second(k=k):
                lat_copy(k, 0).start()
    else:
        for k in cross + inner:
            lat_copy(k, 0).start()
    pairs = (
        (w_query_hbm, w_query),
        (w_kv_hbm, w_kv),
        (w_out_hbm, w_out),
        (w_up_hbm, w_up),
        (w_down_hbm, w_down),
        (w_vocab_hbm, w_vocab),
    )
    for index, (src, dst) in enumerate(pairs):
        start_local(src, dst, w_sem.at[index])

    for k in range(1, group):
        q_copy(k).start()
        t_copy(k).start()
        m_copy(k).start()
    for k in cross + inner:
        lat_copy(k, 1).start()

    for copy in local:
        copy.wait()
    for k in range(1, group):
        q_copy(k).wait_recv()
        t_copy(k).wait_recv()
        m_copy(k).wait_recv()

    rows_dev = q_buf.shape[2]
    width = q_buf.shape[3]
    rows_all = group * rows_dev
    lat_dev = lat_buf.shape[2]
    lat_split, row_split = LAT_SPLIT, ROW_SPLIT
    lat_width = lat_buf.shape[3]
    head_dim = width // HEADS
    scale_factor = float(head_dim) ** (-0.5)
    vocab = w_vocab.shape[0]
    lanes = 128
    acc[...] = jnp.zeros_like(acc)

    columns = []
    for k in range(group):
        code = (t_buf[k] + vocab * m_buf[k]).astype(jnp.float32)
        pad = -rows_dev % lanes
        if pad:
            code = jnp.concatenate(
                [code, jnp.zeros((code.shape[0], pad), jnp.float32)], axis=1
            )
        columns.append(code.T[:rows_dev])
    code_cols = jnp.concatenate(columns, axis=0)

    def one_sequence(i, carry):
        seq_queries = q_buf[:, i].reshape(rows_all, width)
        query_all = dot(seq_queries, w_query[...]).astype(jnp.bfloat16)

        chunk = 256
        step = n_pos // lat_split
        lat_rows = step * lat_dev
        for part in reversed(range(lat_split)):
            for k in reversed(range(part * step, (part + 1) * step)):
                if k == 0:
                    lat_local(i).wait()
                else:
                    lat_copy(k, i).wait_recv()
            field = lat_buf[i, part * step : (part + 1) * step].astype(jnp.float32)
            field = field.reshape(lat_rows, lat_width)
            normed_lat = layer_norm(field, kv_gain[...].reshape(1, lat_width)).astype(jnp.bfloat16)
            for start in range(0, 2 * width, chunk):
                kv_buf[part * lat_rows : (part + 1) * lat_rows, start : start + chunk] = dot(
                    normed_lat, w_kv[:, start : start + chunk]
                ).astype(jnp.bfloat16)

        for part in reversed(range(row_split)):
            decode(i, part, query_all)
        return carry

    def decode(i, part, query_all):
        members = group // row_split
        begin_slot = part * members
        rows = members * rows_dev
        begin_row = begin_slot * rows_dev
        query_proj = query_all[begin_row : begin_row + rows]
        seq_queries = q_buf[begin_slot : begin_slot + members, i].reshape(rows, width)
        code_all = code_cols[begin_row : begin_row + rows]

        tiles = [None] * (width // lanes)
        for h in range(HEADS):
            low, high = h * head_dim, (h + 1) * head_dim
            first_tile, last_tile = low // lanes, (high - 1) // lanes
            begin, end = first_tile * lanes, (last_tile + 1) * lanes
            lane = lax.broadcasted_iota(jnp.int32, (1, end - begin), 1) + begin
            inside = jnp.logical_and(lane >= low, lane < high).astype(jnp.bfloat16)
            keys = kv_buf[:, begin:end] * inside
            values = kv_buf[:, width + begin : width + end] * inside
            scores = (
                dot_last(query_proj[:, begin:end], keys) * scale_factor
            )
            power = jnp.exp(scores - jnp.max(scores, axis=-1, keepdims=True))
            weights = (power / jnp.sum(power, axis=-1, keepdims=True)).astype(jnp.bfloat16)
            part = dot(weights, values)
            for t in range(first_tile, last_tile + 1):
                piece = part[:, t * lanes - begin : (t + 1) * lanes - begin]
                tiles[t] = piece if tiles[t] is None else tiles[t] + piece
        attended = jnp.concatenate([tile.astype(jnp.bfloat16) for tile in tiles], axis=1)

        first = seq_queries.astype(jnp.float32) + dot(attended, w_out[...])
        normed = layer_norm(first, mlp_gain[...].reshape(1, width)).astype(jnp.bfloat16)
        hidden = jax.nn.gelu(dot(normed, w_up[...])).astype(jnp.bfloat16)
        output = (first + dot(hidden, w_down[...])).astype(jnp.bfloat16)
        full_logits = dot_last(output, w_vocab[...]) + vocab_bias[...].reshape(1, vocab)
        logit_buf[i, begin_slot : begin_slot + members] = full_logits.astype(jnp.bfloat16).reshape(
            members, rows_dev, vocab
        )

        code_lane = lax.broadcasted_iota(jnp.int32, code_all.shape, 1)
        code = jnp.sum(
            jnp.where(code_lane == mine * seqs + i, code_all, 0.0), axis=1, keepdims=True
        )
        weight_mask = (code >= float(vocab)).astype(jnp.float32)
        target = (code - float(vocab) * weight_mask).astype(jnp.int32)
        ids = lax.broadcasted_iota(jnp.int32, full_logits.shape, 1)
        picked = jnp.sum(jnp.where(ids == target, full_logits, 0.0), axis=1, keepdims=True)
        top = jnp.max(full_logits, axis=1, keepdims=True)
        spread = jnp.log(jnp.sum(jnp.exp(full_logits - top), axis=1, keepdims=True))
        cross = top + spread - picked

        for k in range(begin_slot, begin_slot + members):
            @pl.when(i < seqs - 1)
            def send(k=k):
                if k == 0:
                    out_local(i).start()
                else:
                    out_copy(k, i).start()

        loss_sum = jnp.sum(cross * weight_mask, axis=0, keepdims=True)
        mask_sum = jnp.sum(weight_mask, axis=0, keepdims=True)
        place = lax.broadcasted_iota(jnp.int32, acc.shape, 1)
        acc[...] += jnp.where(place == 0, loss_sum, jnp.where(place == 1, mask_sum, 0.0))

    lax.fori_loop(0, seqs, one_sequence, 0)

    n_all = n_pos * n_head
    rank = me * n_head + my_head

    def p_copy(k):
        peer = lax.rem(rank + k, n_all)
        return pltpu.make_async_remote_copy(
            src_ref=part_src,
            dst_ref=part_all.at[rank],
            send_sem=p_send.at[k],
            recv_sem=p_recv.at[k],
            device_id={"pos": peer // n_head, "head": lax.rem(peer, n_head)},
            device_id_type=MESH,
        )

    part = acc[...]
    part_src[...] = part
    part_all[rank] = part
    for k in range(1, n_all):
        p_copy(k).start()
    for k in range(1, group):
        out_copy(k, seqs - 1).start()
    out_local(seqs - 1).start()
    for k in range(1, n_all):
        p_copy(k).wait_recv()
    whole = jnp.sum(part_all[...], axis=0)
    loss_out[...] = whole[:, 0:1] / whole[:, 1:2]

    for k in range(1, n_all):
        p_copy(k).wait_send()
    for k in range(1, group):
        q_copy(k).wait_send()
        t_copy(k).wait_send()
        m_copy(k).wait_send()
    for i in range(seqs):
        for k in range(1, n_pos):
            lat_copy(k, i).wait_send()
        out_local(i).wait()
        for k in range(1, group):
            out_copy(k, i).wait()


def on_device(n_pos, n_head, *args):
    (queries, latents, w_query, kv_gain, w_kv, w_out, mlp_gain, w_up, w_down, w_vocab, vocab_bias, targets, mask) = args
    batch_dev, pos_dev, width = queries.shape
    lat_dev, lat_width = latents.shape[1:]
    vocab = w_vocab.shape[1]
    group = max(1, min(n_pos, batch_dev) // 2)
    seqs = batch_dev // group
    assert n_pos % group == 0 and batch_dev % group == 0
    hbm = pl.BlockSpec(memory_space=pltpu.HBM)
    vmem = pl.BlockSpec(memory_space=pltpu.VMEM)
    dma = pltpu.SemaphoreType.DMA
    bf16, f32 = jnp.bfloat16, jnp.float32
    logits, loss = pl.pallas_call(
        functools.partial(kernel, n_pos, n_head, group, seqs),
        out_shape=(
            jax.ShapeDtypeStruct((batch_dev, pos_dev, vocab), bf16),
            jax.ShapeDtypeStruct((1, 1), f32),
        ),
        in_specs=[hbm, hbm, hbm, vmem, hbm, hbm, vmem, hbm, hbm, hbm, vmem, hbm, hbm],
        out_specs=(pl.BlockSpec(memory_space=pl.ANY), vmem),
        scratch_shapes=[
            pltpu.VMEM(latents.shape, bf16),
            pltpu.VMEM(queries.shape, bf16),
            pltpu.VMEM((seqs, n_pos, lat_dev, lat_width), bf16),
            pltpu.VMEM((group, seqs, pos_dev, width), bf16),
            pltpu.VMEM((group, batch_dev, pos_dev), jnp.int32),
            pltpu.VMEM((group, batch_dev, pos_dev), jnp.int32),
            pltpu.VMEM(w_query.shape, bf16),
            pltpu.VMEM(w_kv.shape, bf16),
            pltpu.VMEM(w_out.shape, bf16),
            pltpu.VMEM(w_up.shape, bf16),
            pltpu.VMEM(w_down.shape, bf16),
            pltpu.VMEM(w_vocab.shape[::-1], bf16),
            pltpu.VMEM((n_pos * lat_dev, 2 * width), bf16),
            pltpu.VMEM((seqs, group, pos_dev, vocab), bf16),
            pltpu.VMEM((1, 128), f32),
            pltpu.VMEM((1, 128), f32),
            pltpu.VMEM((n_pos * n_head, 1, 128), f32),
            dma((seqs, n_pos)),
            dma((seqs, n_pos)),
            dma((group,)),
            dma((group,)),
            dma((group,)),
            dma((group,)),
            dma((group,)),
            dma((group,)),
            dma((seqs, group)),
            dma((seqs, group)),
            dma((n_pos * n_head,)),
            dma((n_pos * n_head,)),
            dma((6,)),
            dma((2,)),
            pltpu.SemaphoreType.REGULAR((2,)),
        ],
        compiler_params=pltpu.CompilerParams(
            collective_id=0, has_side_effects=True, vmem_limit_bytes=60 * 1024 * 1024
        ),
    )(
        queries,
        latents,
        w_query,
        kv_gain,
        w_kv,
        w_out,
        mlp_gain,
        w_up,
        w_down,
        w_vocab.T,
        vocab_bias,
        targets,
        mask,
    )
    return (logits, loss.reshape(()))


def solution(mesh):
    in_specs = (
        P("head", "pos", None),
        P("head", "pos", None),
        P(),
        P(),
        P(),
        P(),
        P(),
        P(),
        P(),
        P(),
        P(),
        P("head", "pos"),
        P("head", "pos"),
    )
    out_specs = (P("head", "pos", None), P())
    return jax.shard_map(
        functools.partial(on_device, mesh.shape["pos"], mesh.shape["head"]),
        mesh=mesh,
        in_specs=in_specs,
        out_specs=out_specs,
        check_vma=False,
    )
```

```python
import functools
import math

import jax
import jax.numpy as jnp
from jax import lax
from jax.experimental import pallas as pl
from jax.experimental.pallas import tpu as pltpu
from jax.sharding import PartitionSpec as P

HEADS = 8
LAT_SPLIT = 2
LANES = 128
epsilon = 1e-05
MESH = pl.DeviceIdType.MESH


def layer_norm(field, gain, axis):
    centre = field - jnp.mean(field, axis=axis, keepdims=True)
    spread = jnp.mean(centre * centre, axis=axis, keepdims=True)
    return centre * lax.rsqrt(spread + epsilon) * gain


def dot(left, right):
    return jnp.dot(left, right, preferred_element_type=jnp.float32)


def dot_parts(left, right, cut):
    return jnp.concatenate([dot(left[:cut], right), dot(left[cut:], right)], axis=0)


def head_span(h, head_dim):
    low, high = h * head_dim, (h + 1) * head_dim
    begin = low // LANES * LANES
    end = -(-high // LANES) * LANES
    return low, high, begin, end


def kernel(
    n_pos,
    n_head,
    group,
    seqs,
    queries,
    latents,
    w_query_hbm,
    kv_gain,
    w_kv_hbm,
    w_out_hbm,
    mlp_gain,
    w_up_hbm,
    w_down_hbm,
    w_vocab_hbm,
    vocab_bias,
    targets,
    mask,
    out,
    loss_out,
    lat_stage,
    q_stage,
    lat_buf,
    q_buf,
    t_buf,
    m_buf,
    w_query,
    w_kv,
    w_out,
    w_up,
    w_down,
    w_vocab,
    w_query_t,
    w_out_t,
    w_up_t,
    w_down_t,
    gain_col,
    bias_row,
    bias_col,
    x_t,
    q_pad,
    norm_buf,
    k_buf,
    v_t,
    score_buf,
    top_buf,
    total_buf,
    power_buf,
    att_t,
    turn_buf,
    logit_buf,
    acc,
    part_src,
    part_all,
    lat_send,
    lat_recv,
    q_own,
    q_send,
    q_recv,
    t_send,
    t_recv,
    m_send,
    m_recv,
    out_send,
    out_recv,
    p_send,
    p_recv,
    w_sem,
    stage_sem,
    stage_sems,
):
    me = lax.axis_index("pos")
    my_head = lax.axis_index("head")
    mine = lax.rem(me, group)
    base = me - mine

    def pos_peer(k):
        return lax.rem(base + (k // group) * group, n_pos) + lax.rem(mine + k % group, group)

    def group_peer(k):
        return base + lax.rem(mine + k, group)

    def group_source(k):
        return base + lax.rem(mine + group - k, group)

    block = max(1, group // 2)
    n_rows = n_pos // block
    staged_entry = 2 < n_rows <= 4
    row = me // block
    spot = lax.rem(me, block)

    def near(peer):
        gap = peer // block - row
        return jnp.logical_and(gap >= -1, gap <= 1)

    def signal_near(semaphore):
        for k in range(1, block):
            pl.semaphore_signal(
                semaphore,
                inc=1,
                device_id={"pos": row * block + lax.rem(spot + k, block)},
                device_id_type=MESH,
            )
        for shift, inside in ((-1, row > 0), (1, row < n_rows - 1)):

            @pl.when(inside)
            def neighbours(shift=shift):
                for k in range(block):
                    pl.semaphore_signal(
                        semaphore,
                        inc=1,
                        device_id={"pos": (row + shift) * block + k},
                        device_id_type=MESH,
                    )

    barrier = pltpu.get_barrier_semaphore()
    for k in range(1, n_head):
        pl.semaphore_signal(
            barrier, inc=1, device_id={"head": lax.rem(my_head + k, n_head)}, device_id_type=MESH
        )
    if staged_entry:
        signal_near(barrier)
        ends = (row > 0).astype(jnp.int32) + (row < n_rows - 1).astype(jnp.int32)
        n_near = block - 1 + block * ends
    else:
        for k in range(1, n_pos):
            pl.semaphore_signal(
                barrier, inc=1, device_id={"pos": pos_peer(k)}, device_id_type=MESH
            )
        n_near = n_pos - 1

    staged = (
        pltpu.make_async_copy(latents, lat_stage, stage_sem.at[0]),
        pltpu.make_async_copy(queries, q_stage, stage_sem.at[1]),
    )
    for copy in staged:
        copy.start()
    local = []

    def start_local(src, dst, sem):
        copy = pltpu.make_async_copy(src, dst, sem)
        copy.start()
        local.append(copy)

    start_local(queries.at[pl.ds(mine * seqs, seqs)], q_buf.at[0], q_own)
    start_local(targets, t_buf.at[0], t_recv.at[0])
    start_local(mask, m_buf.at[0], m_recv.at[0])
    def lat_copy(k, i):
        peer = pos_peer(k)
        return pltpu.make_async_remote_copy(
            src_ref=lat_stage.at[lax.rem(peer, group) * seqs + i],
            dst_ref=lat_buf.at[i, k],
            send_sem=lat_send.at[i, k],
            recv_sem=lat_recv.at[i, k],
            device_id={"pos": peer},
            device_id_type=MESH,
        )

    def lat_local(i):
        return pltpu.make_async_copy(
            latents.at[mine * seqs + i], lat_buf.at[i, 0], lat_recv.at[i, 0]
        )

    def group_copy(k, src, dst, send, recv):
        return pltpu.make_async_remote_copy(
            src_ref=src,
            dst_ref=dst,
            send_sem=send.at[k],
            recv_sem=recv.at[k],
            device_id={"pos": group_peer(k)},
            device_id_type=MESH,
        )

    def q_copy(k, i):
        peer = lax.rem(mine + k, group)
        return group_copy(
            k, q_stage.at[peer * seqs + i], q_buf.at[k, i], q_send.at[i], q_recv.at[i]
        )

    def t_copy(k):
        return group_copy(k, targets, t_buf.at[k], t_send, t_recv)

    def m_copy(k):
        return group_copy(k, mask, m_buf.at[k], m_send, m_recv)

    def out_copy(k, i):
        return pltpu.make_async_remote_copy(
            src_ref=logit_buf.at[i, k],
            dst_ref=out.at[mine * seqs + i],
            send_sem=out_send.at[i, k],
            recv_sem=out_recv.at[i, k],
            device_id={"pos": group_source(k)},
            device_id_type=MESH,
        )

    def out_local(i):
        return pltpu.make_async_copy(
            logit_buf.at[i, 0], out.at[mine * seqs + i], out_recv.at[i, 0]
        )

    for i in range(seqs):
        lat_local(i).start()

    pl.semaphore_wait(barrier, n_near + n_head - 1)
    for copy in staged:
        copy.wait()

    cross = tuple(range(group, n_pos))
    inner = tuple(range(1, group))
    if staged_entry:
        for k in cross + inner:

            @pl.when(near(pos_peer(k)))
            def first(k=k):
                lat_copy(k, 0).start()

        for stage in range(n_rows - 2):
            signal_near(stage_sems.at[stage])
            pl.semaphore_wait(stage_sems.at[stage], n_near)
        for k in cross + inner:

            @pl.when(jnp.logical_not(near(pos_peer(k))))
            def second(k=k):
                lat_copy(k, 0).start()
    else:
        for k in cross + inner:
            lat_copy(k, 0).start()
    pairs = (
        (w_query_hbm, w_query),
        (w_kv_hbm, w_kv),
        (w_out_hbm, w_out),
        (w_up_hbm, w_up),
        (w_down_hbm, w_down),
        (w_vocab_hbm, w_vocab),
    )
    for index, (src, dst) in enumerate(pairs):
        start_local(src, dst, w_sem.at[index])

    for k in range(1, group):
        t_copy(k).start()
        m_copy(k).start()
    for i in range(seqs):
        if i > 0:
            for k in cross:

                @pl.when(jnp.logical_not(near(pos_peer(k))))
                def third(k=k, i=i):
                    lat_copy(k, i).start()

        for k in range(1, group):
            q_copy(k, i).start()
        if i > 0:
            for k in cross:

                @pl.when(near(pos_peer(k)))
                def fourth(k=k, i=i):
                    lat_copy(k, i).start()

            for k in inner:
                lat_copy(k, i).start()

    rows_dev = q_buf.shape[2]
    width = q_buf.shape[3]
    rows_all = group * rows_dev
    lat_dev = lat_buf.shape[2]
    lat_width = lat_buf.shape[3]
    head_dim = width // HEADS
    power_scale = float(head_dim) ** (-0.5) * math.log2(math.e)
    vocab = w_vocab.shape[0]

    for copy in local:
        copy.wait()
    for raw, turned in (
        (w_query, w_query_t),
        (w_out, w_out_t),
        (w_up, w_up_t),
        (w_down, w_down_t),
    ):
        turned[...] = raw[...].T
    gain_col[...] = jnp.broadcast_to(mlp_gain[...].reshape(1, width), (LANES, width)).T
    turn_buf[...] = jnp.zeros_like(turn_buf)
    bias_row[...] = jnp.zeros_like(bias_row)
    bias_row[:, :vocab] = vocab_bias[...].reshape(1, vocab)
    bias_col[...] = jnp.broadcast_to(bias_row[...], (LANES, bias_row.shape[1])).T

    def wide(column):
        return jnp.concatenate([column] * (rows_all // LANES), axis=1)

    for k in range(1, group):
        t_copy(k).wait_recv()
        m_copy(k).wait_recv()

    def prepare(i):
        for k in range(1, group):
            q_copy(k, i).wait_recv()
        turned = q_buf[:, i].reshape(rows_all, width).T
        x_t[i] = turned.astype(jnp.float32)
        query_t = dot(w_query_t[...], turned).astype(jnp.bfloat16)
        for h in range(HEADS):
            low, high, begin, end = head_span(h, head_dim)
            if low > begin:
                q_pad[i, h, : low - begin] = jnp.zeros((low - begin, rows_all), jnp.bfloat16)
            q_pad[i, h, low - begin : high - begin] = query_t[low:high]
            if end > high:
                q_pad[i, h, high - begin : end - begin] = jnp.zeros(
                    (end - high, rows_all), jnp.bfloat16
                )

    acc[...] = jnp.zeros_like(acc)

    slots = n_pos // LAT_SPLIT
    lat_rows = slots * lat_dev
    some = max(1, min(slots, 64 // lat_dev))
    chunk = 256

    def one_sequence(i, carry):
        prepare(i)
        for part in reversed(range(LAT_SPLIT)):
            base_row = part * lat_rows
            for start in range(part * slots, (part + 1) * slots, some):
                for k in range(start, start + some):
                    if k == 0:
                        lat_local(i).wait()
                    else:
                        lat_copy(k, i).wait_recv()
                field = lat_buf[i, start : start + some].astype(jnp.float32)
                field = field.reshape(some * lat_dev, lat_width)
                norm_buf[start * lat_dev : (start + some) * lat_dev] = layer_norm(
                    field, kv_gain[...].reshape(1, lat_width), 1
                ).astype(jnp.bfloat16)
            normed_lat = norm_buf[base_row : base_row + lat_rows]
            for start in range(0, 2 * width, chunk):
                block_kv = dot(normed_lat, w_kv[:, start : start + chunk]).astype(jnp.bfloat16)
                if start < width:
                    k_buf[base_row : base_row + lat_rows, start : start + chunk] = block_kv
                else:
                    v_t[start - width : start - width + chunk, base_row : base_row + lat_rows] = (
                        block_kv.T
                    )

        for h in range(HEADS):
            low, high, begin, end = head_span(h, head_dim)
            scores = dot(k_buf[:, begin:end], q_pad[i, h, : end - begin])
            score_buf[h] = scores
            top_buf[h : h + 1] = jnp.max(scores, axis=0, keepdims=True)
        for h in range(HEADS):
            power = jnp.exp2((score_buf[h] - top_buf[h : h + 1]) * power_scale)
            total_buf[h : h + 1] = jnp.sum(power, axis=0, keepdims=True)
            power_buf[h] = power.astype(jnp.bfloat16)
        for h in range(HEADS):
            low, high = h * head_dim, (h + 1) * head_dim
            mixed = dot(v_t[low:high], power_buf[h])
            att_t[low:high] = (mixed * (1.0 / total_buf[h : h + 1])).astype(jnp.bfloat16)

        half = width // 2
        first = x_t[i] + dot_parts(w_out_t, att_t[...], half)
        normed = layer_norm(first, wide(gain_col[...]), 0).astype(jnp.bfloat16)
        hidden = jax.nn.gelu(dot_parts(w_up_t, normed, half)).astype(jnp.bfloat16)
        output = (first + dot_parts(w_down_t, hidden, half)).astype(jnp.bfloat16)
        full_logits = dot_parts(w_vocab, output, LANES) + wide(bias_col[:vocab])
        turn_buf[:vocab] = full_logits
        logit_buf[i] = (
            turn_buf[...].T[:, :vocab].astype(jnp.bfloat16).reshape(group, rows_dev, vocab)
        )

        line = mine * seqs + i
        target = jnp.concatenate([t_buf[k, pl.ds(line, 1)] for k in range(group)], axis=1)
        weight = jnp.concatenate([m_buf[k, pl.ds(line, 1)] for k in range(group)], axis=1)
        weight = weight.astype(jnp.float32)
        ids = lax.broadcasted_iota(jnp.int32, full_logits.shape, 0)
        picked = jnp.sum(jnp.where(ids == target, full_logits, 0.0), axis=0, keepdims=True)
        top = jnp.max(full_logits, axis=0, keepdims=True)
        spread = jnp.log(jnp.sum(jnp.exp(full_logits - top), axis=0, keepdims=True))
        cross_loss = (top + spread - picked) * weight
        for start in range(0, rows_all, LANES):
            acc[:, :LANES] += cross_loss[:, start : start + LANES]
            acc[:, LANES:] += weight[:, start : start + LANES]

        for k in range(group):

            @pl.when(i < seqs - 1)
            def send(k=k):
                if k == 0:
                    out_local(i).start()
                else:
                    out_copy(k, i).start()

        return carry

    lax.fori_loop(0, seqs, one_sequence, 0)

    n_all = n_pos * n_head
    rank = me * n_head + my_head

    def p_copy(k):
        peer = lax.rem(rank + k, n_all)
        return pltpu.make_async_remote_copy(
            src_ref=part_src,
            dst_ref=part_all.at[rank],
            send_sem=p_send.at[k],
            recv_sem=p_recv.at[k],
            device_id={"pos": peer // n_head, "head": lax.rem(peer, n_head)},
            device_id_type=MESH,
        )

    part = acc[...]
    part_src[...] = part
    part_all[rank] = part
    for k in range(1, n_all):
        p_copy(k).start()
    for k in range(1, group):
        out_copy(k, seqs - 1).start()
    out_local(seqs - 1).start()
    for k in range(1, n_all):
        p_copy(k).wait_recv()
    whole = jnp.sum(part_all[...], axis=0)
    loss_out[...] = jnp.sum(whole[:, :LANES], axis=1, keepdims=True) / jnp.sum(
        whole[:, LANES:], axis=1, keepdims=True
    )

    for k in range(1, n_all):
        p_copy(k).wait_send()
    for k in range(1, group):
        for i in range(seqs):
            q_copy(k, i).wait_send()
        t_copy(k).wait_send()
        m_copy(k).wait_send()
    for i in range(seqs):
        for k in range(1, n_pos):
            lat_copy(k, i).wait_send()
        out_local(i).wait()
        for k in range(1, group):
            out_copy(k, i).wait()


def on_device(n_pos, n_head, *args):
    (queries, latents, w_query, kv_gain, w_kv, w_out, mlp_gain, w_up, w_down, w_vocab, vocab_bias, targets, mask) = args
    batch_dev, pos_dev, width = queries.shape
    lat_dev, lat_width = latents.shape[1:]
    vocab = w_vocab.shape[1]
    group = max(1, min(n_pos, batch_dev) // 2)
    seqs = batch_dev // group
    assert n_pos % group == 0 and batch_dev % group == 0
    rows_all = group * pos_dev
    assert rows_all % LANES == 0 and n_pos % LAT_SPLIT == 0
    vocab_pad = -(-vocab // LANES) * LANES
    hbm = pl.BlockSpec(memory_space=pltpu.HBM)
    vmem = pl.BlockSpec(memory_space=pltpu.VMEM)
    dma = pltpu.SemaphoreType.DMA
    bf16, f32 = jnp.bfloat16, jnp.float32
    logits, loss = pl.pallas_call(
        functools.partial(kernel, n_pos, n_head, group, seqs),
        out_shape=(
            jax.ShapeDtypeStruct((batch_dev, pos_dev, vocab), bf16),
            jax.ShapeDtypeStruct((1, 1), f32),
        ),
        in_specs=[hbm, hbm, hbm, vmem, hbm, hbm, vmem, hbm, hbm, hbm, vmem, hbm, hbm],
        out_specs=(pl.BlockSpec(memory_space=pl.ANY), vmem),
        scratch_shapes=[
            pltpu.VMEM(latents.shape, bf16),
            pltpu.VMEM(queries.shape, bf16),
            pltpu.VMEM((seqs, n_pos, lat_dev, lat_width), bf16),
            pltpu.VMEM((group, seqs, pos_dev, width), bf16),
            pltpu.VMEM((group, batch_dev, pos_dev), jnp.int32),
            pltpu.VMEM((group, batch_dev, pos_dev), jnp.int32),
            pltpu.VMEM(w_query.shape, bf16),
            pltpu.VMEM(w_kv.shape, bf16),
            pltpu.VMEM(w_out.shape, bf16),
            pltpu.VMEM(w_up.shape, bf16),
            pltpu.VMEM(w_down.shape, bf16),
            pltpu.VMEM(w_vocab.shape[::-1], bf16),
            pltpu.VMEM(w_query.shape[::-1], bf16),
            pltpu.VMEM(w_out.shape[::-1], bf16),
            pltpu.VMEM(w_up.shape[::-1], bf16),
            pltpu.VMEM(w_down.shape[::-1], bf16),
            pltpu.VMEM((width, LANES), f32),
            pltpu.VMEM((1, vocab_pad), f32),
            pltpu.VMEM((vocab_pad, LANES), f32),
            pltpu.VMEM((seqs, width, rows_all), f32),
            pltpu.VMEM((seqs, HEADS, 2 * LANES, rows_all), bf16),
            pltpu.VMEM((n_pos * lat_dev, lat_width), bf16),
            pltpu.VMEM((n_pos * lat_dev, width), bf16),
            pltpu.VMEM((width, n_pos * lat_dev), bf16),
            pltpu.VMEM((HEADS, n_pos * lat_dev, rows_all), f32),
            pltpu.VMEM((HEADS, rows_all), f32),
            pltpu.VMEM((HEADS, rows_all), f32),
            pltpu.VMEM((HEADS, n_pos * lat_dev, rows_all), bf16),
            pltpu.VMEM((width, rows_all), bf16),
            pltpu.VMEM((vocab_pad, rows_all), f32),
            pltpu.VMEM((seqs, group, pos_dev, vocab), bf16),
            pltpu.VMEM((1, 2 * LANES), f32),
            pltpu.VMEM((1, 2 * LANES), f32),
            pltpu.VMEM((n_pos * n_head, 1, 2 * LANES), f32),
            dma((seqs, n_pos)),
            dma((seqs, n_pos)),
            pltpu.SemaphoreType.DMA,
            dma((seqs, group)),
            dma((seqs, group)),
            dma((group,)),
            dma((group,)),
            dma((group,)),
            dma((group,)),
            dma((seqs, group)),
            dma((seqs, group)),
            dma((n_pos * n_head,)),
            dma((n_pos * n_head,)),
            dma((6,)),
            dma((2,)),
            pltpu.SemaphoreType.REGULAR((2,)),
        ],
        compiler_params=pltpu.CompilerParams(
            collective_id=0, has_side_effects=True, vmem_limit_bytes=60 * 1024 * 1024
        ),
    )(
        queries,
        latents,
        w_query,
        kv_gain,
        w_kv,
        w_out,
        mlp_gain,
        w_up,
        w_down,
        w_vocab.T,
        vocab_bias,
        targets,
        mask,
    )
    return (logits, loss.reshape(()))


def solution(mesh):
    in_specs = (
        P("head", "pos", None),
        P("head", "pos", None),
        P(),
        P(),
        P(),
        P(),
        P(),
        P(),
        P(),
        P(),
        P(),
        P("head", "pos"),
        P("head", "pos"),
    )
    out_specs = (P("head", "pos", None), P())
    return jax.shard_map(
        functools.partial(on_device, mesh.shape["pos"], mesh.shape["head"]),
        mesh=mesh,
        in_specs=in_specs,
        out_specs=out_specs,
        check_vma=False,
    )
```

```python
import functools
import math

import jax
import jax.numpy as jnp
from jax import lax
from jax.experimental import pallas as pl
from jax.experimental.pallas import tpu as pltpu
from jax.sharding import PartitionSpec as P

HEADS = 8
LAT_SPLIT = 2
LANES = 128
epsilon = 1e-05
MESH = pl.DeviceIdType.MESH


def layer_norm(field, gain, axis):
    centre = field - jnp.mean(field, axis=axis, keepdims=True)
    spread = jnp.mean(centre * centre, axis=axis, keepdims=True)
    return centre * lax.rsqrt(spread + epsilon) * gain


def dot(left, right):
    return jnp.dot(left, right, preferred_element_type=jnp.float32)


def dot_parts(left, right, cut):
    return jnp.concatenate([dot(left[:cut], right), dot(left[cut:], right)], axis=0)


def head_span(h, head_dim):
    low, high = h * head_dim, (h + 1) * head_dim
    begin = low // LANES * LANES
    end = -(-high // LANES) * LANES
    return low, high, begin, end


def kernel(
    n_pos,
    n_head,
    group,
    seqs,
    queries,
    latents,
    w_query_hbm,
    kv_gain,
    w_kv_hbm,
    w_out_hbm,
    mlp_gain,
    w_up_hbm,
    w_down_hbm,
    w_vocab_hbm,
    vocab_bias,
    targets,
    mask,
    out,
    loss_out,
    lat_stage,
    q_stage,
    lat_buf,
    q_buf,
    t_buf,
    m_buf,
    w_query,
    w_kv,
    w_out,
    w_up,
    w_down,
    w_vocab,
    w_query_t,
    w_out_t,
    w_up_t,
    w_down_t,
    gain_col,
    bias_row,
    bias_col,
    x_t,
    q_pad,
    norm_buf,
    k_buf,
    v_t,
    score_buf,
    top_buf,
    total_buf,
    power_buf,
    att_t,
    turn_buf,
    logit_buf,
    acc,
    part_src,
    part_all,
    lat_send,
    lat_recv,
    q_own,
    q_send,
    q_recv,
    t_send,
    t_recv,
    m_send,
    m_recv,
    out_send,
    out_recv,
    p_send,
    p_recv,
    w_sem,
    stage_sem,
    stage_sems,
):
    me = lax.axis_index("pos")
    my_head = lax.axis_index("head")
    mine = lax.rem(me, group)
    base = me - mine

    def pos_peer(k):
        return lax.rem(base + (k // group) * group, n_pos) + lax.rem(mine + k % group, group)

    def group_peer(k):
        return base + lax.rem(mine + k, group)

    def group_source(k):
        return base + lax.rem(mine + group - k, group)

    block = max(1, group // 2)
    n_rows = n_pos // block
    staged_entry = 2 < n_rows <= 4
    row = me // block
    spot = lax.rem(me, block)

    def near(peer):
        gap = peer // block - row
        return jnp.logical_and(gap >= -1, gap <= 1)

    def signal_near(semaphore):
        for k in range(1, block):
            pl.semaphore_signal(
                semaphore,
                inc=1,
                device_id={"pos": row * block + lax.rem(spot + k, block)},
                device_id_type=MESH,
            )
        for shift, inside in ((-1, row > 0), (1, row < n_rows - 1)):

            @pl.when(inside)
            def neighbours(shift=shift):
                for k in range(block):
                    pl.semaphore_signal(
                        semaphore,
                        inc=1,
                        device_id={"pos": (row + shift) * block + k},
                        device_id_type=MESH,
                    )

    barrier = pltpu.get_barrier_semaphore()
    for k in range(1, n_head):
        pl.semaphore_signal(
            barrier, inc=1, device_id={"head": lax.rem(my_head + k, n_head)}, device_id_type=MESH
        )
    if staged_entry:
        signal_near(barrier)
        ends = (row > 0).astype(jnp.int32) + (row < n_rows - 1).astype(jnp.int32)
        n_near = block - 1 + block * ends
    else:
        for k in range(1, n_pos):
            pl.semaphore_signal(
                barrier, inc=1, device_id={"pos": pos_peer(k)}, device_id_type=MESH
            )
        n_near = n_pos - 1

    staged = (
        pltpu.make_async_copy(latents, lat_stage, stage_sem.at[0]),
        pltpu.make_async_copy(queries, q_stage, stage_sem.at[1]),
    )
    for copy in staged:
        copy.start()
    local = []

    def start_local(src, dst, sem):
        copy = pltpu.make_async_copy(src, dst, sem)
        copy.start()
        local.append(copy)

    start_local(queries.at[pl.ds(mine * seqs, seqs)], q_buf.at[0], q_own)
    start_local(targets, t_buf.at[0], t_recv.at[0])
    start_local(mask, m_buf.at[0], m_recv.at[0])
    def lat_copy(k, i):
        peer = pos_peer(k)
        return pltpu.make_async_remote_copy(
            src_ref=lat_stage.at[lax.rem(peer, group) * seqs + i],
            dst_ref=lat_buf.at[i, k],
            send_sem=lat_send.at[i, k],
            recv_sem=lat_recv.at[i, k],
            device_id={"pos": peer},
            device_id_type=MESH,
        )

    def lat_local(i):
        return pltpu.make_async_copy(
            latents.at[mine * seqs + i], lat_buf.at[i, 0], lat_recv.at[i, 0]
        )

    def group_copy(k, src, dst, send, recv):
        return pltpu.make_async_remote_copy(
            src_ref=src,
            dst_ref=dst,
            send_sem=send.at[k],
            recv_sem=recv.at[k],
            device_id={"pos": group_peer(k)},
            device_id_type=MESH,
        )

    def q_copy(k, i):
        peer = lax.rem(mine + k, group)
        return group_copy(
            k, q_stage.at[peer * seqs + i], q_buf.at[k, i], q_send.at[i], q_recv.at[i]
        )

    def t_copy(k):
        return group_copy(k, targets, t_buf.at[k], t_send, t_recv)

    def m_copy(k):
        return group_copy(k, mask, m_buf.at[k], m_send, m_recv)

    def out_copy(k, i):
        return pltpu.make_async_remote_copy(
            src_ref=logit_buf.at[i, k],
            dst_ref=out.at[mine * seqs + i],
            send_sem=out_send.at[i, k],
            recv_sem=out_recv.at[i, k],
            device_id={"pos": group_source(k)},
            device_id_type=MESH,
        )

    def out_local(i):
        return pltpu.make_async_copy(
            logit_buf.at[i, 0], out.at[mine * seqs + i], out_recv.at[i, 0]
        )

    for i in range(seqs):
        lat_local(i).start()

    pl.semaphore_wait(barrier, n_near + n_head - 1)
    for copy in staged:
        copy.wait()

    cross = tuple(range(group, n_pos))
    inner = tuple(range(1, group))
    if staged_entry:
        for k in cross + inner:

            @pl.when(near(pos_peer(k)))
            def first(k=k):
                lat_copy(k, 0).start()

        for stage in range(n_rows - 2):
            signal_near(stage_sems.at[stage])
            pl.semaphore_wait(stage_sems.at[stage], n_near)
        for k in cross + inner:

            @pl.when(jnp.logical_not(near(pos_peer(k))))
            def second(k=k):
                lat_copy(k, 0).start()
    else:
        for k in cross + inner:
            lat_copy(k, 0).start()
    pairs = (
        (w_query_hbm, w_query),
        (w_kv_hbm, w_kv),
        (w_out_hbm, w_out),
        (w_up_hbm, w_up),
        (w_down_hbm, w_down),
        (w_vocab_hbm, w_vocab),
    )
    for index, (src, dst) in enumerate(pairs):
        start_local(src, dst, w_sem.at[index])

    for k in range(1, group):
        t_copy(k).start()
        m_copy(k).start()
    for i in range(seqs):
        if i > 0:
            for k in cross:

                @pl.when(jnp.logical_not(near(pos_peer(k))))
                def third(k=k, i=i):
                    lat_copy(k, i).start()

        for k in range(1, group):
            q_copy(k, i).start()
        if i > 0:
            for k in cross:

                @pl.when(near(pos_peer(k)))
                def fourth(k=k, i=i):
                    lat_copy(k, i).start()

            for k in inner:
                lat_copy(k, i).start()

    rows_dev = q_buf.shape[2]
    width = q_buf.shape[3]
    rows_all = group * rows_dev
    lat_dev = lat_buf.shape[2]
    lat_width = lat_buf.shape[3]
    head_dim = width // HEADS
    power_scale = float(head_dim) ** (-0.5) * math.log2(math.e)
    vocab = w_vocab.shape[0]

    for copy in local:
        copy.wait()
    for raw, turned in (
        (w_query, w_query_t),
        (w_out, w_out_t),
        (w_up, w_up_t),
        (w_down, w_down_t),
    ):
        turned[...] = raw[...].T
    gain_col[...] = jnp.broadcast_to(mlp_gain[...].reshape(1, width), (LANES, width)).T
    turn_buf[...] = jnp.zeros_like(turn_buf)
    bias_row[...] = jnp.zeros_like(bias_row)
    bias_row[:, :vocab] = vocab_bias[...].reshape(1, vocab)
    bias_col[...] = jnp.broadcast_to(bias_row[...], (LANES, bias_row.shape[1])).T

    def wide(column):
        return jnp.concatenate([column] * (rows_all // LANES), axis=1)

    for k in range(1, group):
        t_copy(k).wait_recv()
        m_copy(k).wait_recv()

    def prepare(i):
        for k in range(1, group):
            q_copy(k, i).wait_recv()
        turned = q_buf[:, i].reshape(rows_all, width).T
        x_t[i] = turned.astype(jnp.float32)
        query_t = dot(w_query_t[...], turned).astype(jnp.bfloat16)
        for h in range(HEADS):
            low, high, begin, end = head_span(h, head_dim)
            if low > begin:
                q_pad[i, h, : low - begin] = jnp.zeros((low - begin, rows_all), jnp.bfloat16)
            q_pad[i, h, low - begin : high - begin] = query_t[low:high]
            if end > high:
                q_pad[i, h, high - begin : end - begin] = jnp.zeros(
                    (end - high, rows_all), jnp.bfloat16
                )

    acc[...] = jnp.zeros_like(acc)

    slots = n_pos // LAT_SPLIT
    lat_rows = slots * lat_dev
    some = max(1, min(slots, 64 // lat_dev))
    chunk = 256

    def hand_over(i):
        logit_buf[i] = (
            turn_buf[i].T[:, :vocab].astype(jnp.bfloat16).reshape(group, rows_dev, vocab)
        )
        for k in range(1, group):
            out_copy(k, i).start()
        out_local(i).start()

    def one_sequence(i, carry):
        prepare(i)

        @pl.when(i > 0)
        def earlier():
            hand_over(i - 1)

        for part in reversed(range(LAT_SPLIT)):
            base_row = part * lat_rows
            for start in range(part * slots, (part + 1) * slots, some):
                for k in range(start, start + some):
                    if k == 0:
                        lat_local(i).wait()
                    else:
                        lat_copy(k, i).wait_recv()
                field = lat_buf[i, start : start + some].astype(jnp.float32)
                field = field.reshape(some * lat_dev, lat_width)
                norm_buf[start * lat_dev : (start + some) * lat_dev] = layer_norm(
                    field, kv_gain[...].reshape(1, lat_width), 1
                ).astype(jnp.bfloat16)
            normed_lat = norm_buf[base_row : base_row + lat_rows]
            for start in range(0, 2 * width, chunk):
                block_kv = dot(normed_lat, w_kv[:, start : start + chunk]).astype(jnp.bfloat16)
                if start < width:
                    k_buf[base_row : base_row + lat_rows, start : start + chunk] = block_kv
                else:
                    v_t[start - width : start - width + chunk, base_row : base_row + lat_rows] = (
                        block_kv.T
                    )

        for h in range(HEADS):
            low, high, begin, end = head_span(h, head_dim)
            scores = dot(k_buf[:, begin:end], q_pad[i, h, : end - begin])
            score_buf[h] = scores
            top_buf[h : h + 1] = jnp.max(scores, axis=0, keepdims=True)
        for h in range(HEADS):
            power = jnp.exp2((score_buf[h] - top_buf[h : h + 1]) * power_scale)
            total_buf[h : h + 1] = jnp.sum(power, axis=0, keepdims=True)
            power_buf[h] = power.astype(jnp.bfloat16)
        for h in range(HEADS):
            low, high = h * head_dim, (h + 1) * head_dim
            mixed = dot(v_t[low:high], power_buf[h])
            att_t[low:high] = (mixed * (1.0 / total_buf[h : h + 1])).astype(jnp.bfloat16)

        half = width // 2
        first = x_t[i] + dot_parts(w_out_t, att_t[...], half)
        normed = layer_norm(first, wide(gain_col[...]), 0).astype(jnp.bfloat16)
        hidden = jax.nn.gelu(dot_parts(w_up_t, normed, half)).astype(jnp.bfloat16)
        output = (first + dot_parts(w_down_t, hidden, half)).astype(jnp.bfloat16)
        full_logits = dot_parts(w_vocab, output, LANES) + wide(bias_col[:vocab])
        turn_buf[i, :vocab] = full_logits
        line = mine * seqs + i
        target = jnp.concatenate([t_buf[k, pl.ds(line, 1)] for k in range(group)], axis=1)
        weight = jnp.concatenate([m_buf[k, pl.ds(line, 1)] for k in range(group)], axis=1)
        weight = weight.astype(jnp.float32)
        ids = lax.broadcasted_iota(jnp.int32, full_logits.shape, 0)
        picked = jnp.sum(jnp.where(ids == target, full_logits, 0.0), axis=0, keepdims=True)
        top = jnp.max(full_logits, axis=0, keepdims=True)
        spread = jnp.log(jnp.sum(jnp.exp(full_logits - top), axis=0, keepdims=True))
        cross_loss = (top + spread - picked) * weight
        for start in range(0, rows_all, LANES):
            acc[:, :LANES] += cross_loss[:, start : start + LANES]
            acc[:, LANES:] += weight[:, start : start + LANES]

        return carry

    lax.fori_loop(0, seqs, one_sequence, 0)

    n_all = n_pos * n_head
    rank = me * n_head + my_head

    swaps = [k // 2 if k % 2 == 0 else n_all - 1 - k // 2 for k in range(n_all)]

    def p_peer(k):
        return lax.rem(2 * n_all - 1 - rank + k, n_all)

    def p_each(act):
        for k in swaps:

            @pl.when(p_peer(k) != rank)
            def other(k=k):
                act(p_copy(k))

    def p_copy(k):
        peer = p_peer(k)
        return pltpu.make_async_remote_copy(
            src_ref=part_src,
            dst_ref=part_all.at[rank],
            send_sem=p_send.at[k],
            recv_sem=p_recv.at[k],
            device_id={"pos": peer // n_head, "head": lax.rem(peer, n_head)},
            device_id_type=MESH,
        )

    part = acc[...]
    part_src[...] = part
    part_all[rank] = part
    p_each(lambda copy: copy.start())
    hand_over(seqs - 1)
    p_each(lambda copy: copy.wait_recv())
    whole = jnp.sum(part_all[...], axis=0)
    loss_out[...] = jnp.sum(whole[:, :LANES], axis=1, keepdims=True) / jnp.sum(
        whole[:, LANES:], axis=1, keepdims=True
    )

    p_each(lambda copy: copy.wait_send())
    for k in range(1, group):
        for i in range(seqs):
            q_copy(k, i).wait_send()
        t_copy(k).wait_send()
        m_copy(k).wait_send()
    for i in range(seqs):
        for k in range(1, n_pos):
            lat_copy(k, i).wait_send()
        out_local(i).wait()
        for k in range(1, group):
            out_copy(k, i).wait()


def on_device(n_pos, n_head, *args):
    (queries, latents, w_query, kv_gain, w_kv, w_out, mlp_gain, w_up, w_down, w_vocab, vocab_bias, targets, mask) = args
    batch_dev, pos_dev, width = queries.shape
    lat_dev, lat_width = latents.shape[1:]
    vocab = w_vocab.shape[1]
    group = max(1, min(n_pos, batch_dev) // 2)
    seqs = batch_dev // group
    assert n_pos % group == 0 and batch_dev % group == 0
    rows_all = group * pos_dev
    assert rows_all % LANES == 0 and n_pos % LAT_SPLIT == 0
    vocab_pad = -(-vocab // LANES) * LANES
    hbm = pl.BlockSpec(memory_space=pltpu.HBM)
    vmem = pl.BlockSpec(memory_space=pltpu.VMEM)
    dma = pltpu.SemaphoreType.DMA
    bf16, f32 = jnp.bfloat16, jnp.float32
    logits, loss = pl.pallas_call(
        functools.partial(kernel, n_pos, n_head, group, seqs),
        out_shape=(
            pltpu.VMEM((batch_dev, pos_dev, vocab), bf16),
            pltpu.VMEM((1, 1), f32),
        ),
        in_specs=[hbm, hbm, hbm, vmem, hbm, hbm, vmem, hbm, hbm, hbm, vmem, hbm, hbm],
        out_specs=(vmem, vmem),
        scratch_shapes=[
            pltpu.VMEM(latents.shape, bf16),
            pltpu.VMEM(queries.shape, bf16),
            pltpu.VMEM((seqs, n_pos, lat_dev, lat_width), bf16),
            pltpu.VMEM((group, seqs, pos_dev, width), bf16),
            pltpu.VMEM((group, batch_dev, pos_dev), jnp.int32),
            pltpu.VMEM((group, batch_dev, pos_dev), jnp.int32),
            pltpu.VMEM(w_query.shape, bf16),
            pltpu.VMEM(w_kv.shape, bf16),
            pltpu.VMEM(w_out.shape, bf16),
            pltpu.VMEM(w_up.shape, bf16),
            pltpu.VMEM(w_down.shape, bf16),
            pltpu.VMEM(w_vocab.shape[::-1], bf16),
            pltpu.VMEM(w_query.shape[::-1], bf16),
            pltpu.VMEM(w_out.shape[::-1], bf16),
            pltpu.VMEM(w_up.shape[::-1], bf16),
            pltpu.VMEM(w_down.shape[::-1], bf16),
            pltpu.VMEM((width, LANES), f32),
            pltpu.VMEM((1, vocab_pad), f32),
            pltpu.VMEM((vocab_pad, LANES), f32),
            pltpu.VMEM((seqs, width, rows_all), f32),
            pltpu.VMEM((seqs, HEADS, 2 * LANES, rows_all), bf16),
            pltpu.VMEM((n_pos * lat_dev, lat_width), bf16),
            pltpu.VMEM((n_pos * lat_dev, width), bf16),
            pltpu.VMEM((width, n_pos * lat_dev), bf16),
            pltpu.VMEM((HEADS, n_pos * lat_dev, rows_all), f32),
            pltpu.VMEM((HEADS, rows_all), f32),
            pltpu.VMEM((HEADS, rows_all), f32),
            pltpu.VMEM((HEADS, n_pos * lat_dev, rows_all), bf16),
            pltpu.VMEM((width, rows_all), bf16),
            pltpu.VMEM((seqs, vocab_pad, rows_all), f32),
            pltpu.VMEM((seqs, group, pos_dev, vocab), bf16),
            pltpu.VMEM((1, 2 * LANES), f32),
            pltpu.VMEM((1, 2 * LANES), f32),
            pltpu.VMEM((n_pos * n_head, 1, 2 * LANES), f32),
            dma((seqs, n_pos)),
            dma((seqs, n_pos)),
            pltpu.SemaphoreType.DMA,
            dma((seqs, group)),
            dma((seqs, group)),
            dma((group,)),
            dma((group,)),
            dma((group,)),
            dma((group,)),
            dma((seqs, group)),
            dma((seqs, group)),
            dma((n_pos * n_head,)),
            dma((n_pos * n_head,)),
            dma((6,)),
            dma((2,)),
            pltpu.SemaphoreType.REGULAR((2,)),
        ],
        compiler_params=pltpu.CompilerParams(
            collective_id=0, has_side_effects=True, vmem_limit_bytes=60 * 1024 * 1024
        ),
    )(
        queries,
        latents,
        w_query,
        kv_gain,
        w_kv,
        w_out,
        mlp_gain,
        w_up,
        w_down,
        w_vocab.T,
        vocab_bias,
        targets,
        mask,
    )
    return (logits, loss.reshape(()))


def solution(mesh):
    in_specs = (
        P("head", "pos", None),
        P("head", "pos", None),
        P(),
        P(),
        P(),
        P(),
        P(),
        P(),
        P(),
        P(),
        P(),
        P("head", "pos"),
        P("head", "pos"),
    )
    out_specs = (P("head", "pos", None), P())
    return jax.shard_map(
        functools.partial(on_device, mesh.shape["pos"], mesh.shape["head"]),
        mesh=mesh,
        in_specs=in_specs,
        out_specs=out_specs,
        check_vma=False,
    )
```

```python
import functools
import math

import jax
import jax.numpy as jnp
from jax import lax
from jax.experimental import pallas as pl
from jax.experimental.pallas import tpu as pltpu
from jax.sharding import PartitionSpec as P

HEADS = 8
LAT_SPLIT = 2
LANES = 128
epsilon = 1e-05
MESH = pl.DeviceIdType.MESH


def layer_norm(field, gain, axis):
    centre = field - jnp.mean(field, axis=axis, keepdims=True)
    spread = jnp.mean(centre * centre, axis=axis, keepdims=True)
    return centre * lax.rsqrt(spread + epsilon) * gain


def dot(left, right):
    return jnp.dot(left, right, preferred_element_type=jnp.float32)


def dot_parts(left, right, cut):
    return jnp.concatenate([dot(left[:cut], right), dot(left[cut:], right)], axis=0)


def head_span(h, head_dim):
    low, high = h * head_dim, (h + 1) * head_dim
    begin = low // LANES * LANES
    end = -(-high // LANES) * LANES
    return low, high, begin, end


def kernel(
    n_pos,
    n_head,
    group,
    seqs,
    queries,
    latents,
    w_query_hbm,
    kv_gain,
    w_kv_hbm,
    w_out_hbm,
    mlp_gain,
    w_up_hbm,
    w_down_hbm,
    w_vocab_hbm,
    vocab_bias,
    targets,
    mask,
    out,
    loss_out,
    lat_stage,
    q_stage,
    lat_buf,
    q_buf,
    t_buf,
    m_buf,
    w_query,
    w_kv,
    w_out,
    w_up,
    w_down,
    w_vocab,
    w_query_t,
    w_out_t,
    w_up_t,
    w_down_t,
    gain_col,
    bias_row,
    bias_col,
    x_t,
    q_pad,
    norm_buf,
    k_buf,
    v_t,
    score_buf,
    top_buf,
    total_buf,
    power_buf,
    att_t,
    turn_buf,
    logit_buf,
    acc,
    part_src,
    part_all,
    lat_send,
    lat_recv,
    q_own,
    q_send,
    q_recv,
    t_send,
    t_recv,
    m_send,
    m_recv,
    out_send,
    out_recv,
    p_send,
    p_recv,
    w_sem,
    stage_sem,
    stage_sems,
):
    me = lax.axis_index("pos")
    my_head = lax.axis_index("head")
    mine = lax.rem(me, group)
    base = me - mine

    def pos_peer(k):
        return lax.rem(base + (k // group) * group, n_pos) + lax.rem(mine + k % group, group)

    def group_peer(k):
        return base + lax.rem(mine + k, group)

    def group_source(k):
        return base + lax.rem(mine + group - k, group)

    block = max(1, group // 2)
    n_rows = n_pos // block
    staged_entry = 2 < n_rows <= 4
    row = me // block
    spot = lax.rem(me, block)

    def near(peer):
        gap = peer // block - row
        return jnp.logical_and(gap >= -1, gap <= 1)

    def signal_near(semaphore):
        for k in range(1, block):
            pl.semaphore_signal(
                semaphore,
                inc=1,
                device_id={"pos": row * block + lax.rem(spot + k, block)},
                device_id_type=MESH,
            )
        for shift, inside in ((-1, row > 0), (1, row < n_rows - 1)):

            @pl.when(inside)
            def neighbours(shift=shift):
                for k in range(block):
                    pl.semaphore_signal(
                        semaphore,
                        inc=1,
                        device_id={"pos": (row + shift) * block + k},
                        device_id_type=MESH,
                    )

    barrier = pltpu.get_barrier_semaphore()
    for k in range(1, n_head):
        pl.semaphore_signal(
            barrier, inc=1, device_id={"head": lax.rem(my_head + k, n_head)}, device_id_type=MESH
        )
    if staged_entry:
        signal_near(barrier)
        ends = (row > 0).astype(jnp.int32) + (row < n_rows - 1).astype(jnp.int32)
        n_near = block - 1 + block * ends
    else:
        for k in range(1, n_pos):
            pl.semaphore_signal(
                barrier, inc=1, device_id={"pos": pos_peer(k)}, device_id_type=MESH
            )
        n_near = n_pos - 1

    staged = (
        pltpu.make_async_copy(latents, lat_stage, stage_sem.at[0]),
        pltpu.make_async_copy(queries, q_stage, stage_sem.at[1]),
    )
    for copy in staged:
        copy.start()
    local = []

    def start_local(src, dst, sem):
        copy = pltpu.make_async_copy(src, dst, sem)
        copy.start()
        local.append(copy)

    start_local(queries.at[pl.ds(mine * seqs, seqs)], q_buf.at[0], q_own)
    start_local(targets, t_buf.at[0], t_recv.at[0])
    start_local(mask, m_buf.at[0], m_recv.at[0])
    def lat_copy(k, i):
        peer = pos_peer(k)
        return pltpu.make_async_remote_copy(
            src_ref=lat_stage.at[lax.rem(peer, group) * seqs + i],
            dst_ref=lat_buf.at[i, k],
            send_sem=lat_send.at[i, k],
            recv_sem=lat_recv.at[i, k],
            device_id={"pos": peer},
            device_id_type=MESH,
        )

    def lat_local(i):
        return pltpu.make_async_copy(
            latents.at[mine * seqs + i], lat_buf.at[i, 0], lat_recv.at[i, 0]
        )

    def group_copy(k, src, dst, send, recv):
        return pltpu.make_async_remote_copy(
            src_ref=src,
            dst_ref=dst,
            send_sem=send.at[k],
            recv_sem=recv.at[k],
            device_id={"pos": group_peer(k)},
            device_id_type=MESH,
        )

    def q_copy(k, i):
        peer = lax.rem(mine + k, group)
        return group_copy(
            k, q_stage.at[peer * seqs + i], q_buf.at[k, i], q_send.at[i], q_recv.at[i]
        )

    def t_copy(k):
        return group_copy(k, targets, t_buf.at[k], t_send, t_recv)

    def m_copy(k):
        return group_copy(k, mask, m_buf.at[k], m_send, m_recv)

    def out_copy(k, i):
        return pltpu.make_async_remote_copy(
            src_ref=logit_buf.at[i, k],
            dst_ref=out.at[mine * seqs + i],
            send_sem=out_send.at[i, k],
            recv_sem=out_recv.at[i, k],
            device_id={"pos": group_source(k)},
            device_id_type=MESH,
        )

    def out_local(i):
        return pltpu.make_async_copy(
            logit_buf.at[i, 0], out.at[mine * seqs + i], out_recv.at[i, 0]
        )

    for i in range(seqs):
        lat_local(i).start()

    pl.semaphore_wait(barrier, n_near + n_head - 1)
    for copy in staged:
        copy.wait()

    cross = tuple(range(group, n_pos))
    inner = tuple(range(1, group))
    if staged_entry:
        for k in cross + inner:

            @pl.when(near(pos_peer(k)))
            def first(k=k):
                lat_copy(k, 0).start()

        for stage in range(n_rows - 2):
            signal_near(stage_sems.at[stage])
            pl.semaphore_wait(stage_sems.at[stage], n_near)
        for k in cross + inner:

            @pl.when(jnp.logical_not(near(pos_peer(k))))
            def second(k=k):
                lat_copy(k, 0).start()
    else:
        for k in cross + inner:
            lat_copy(k, 0).start()
    pairs = (
        (w_query_hbm, w_query),
        (w_kv_hbm, w_kv),
        (w_out_hbm, w_out),
        (w_up_hbm, w_up),
        (w_down_hbm, w_down),
        (w_vocab_hbm, w_vocab),
    )
    for index, (src, dst) in enumerate(pairs):
        start_local(src, dst, w_sem.at[index])

    for k in range(1, group):
        t_copy(k).start()
        m_copy(k).start()
    for i in range(seqs):
        if i > 0:
            for k in cross:

                @pl.when(jnp.logical_not(near(pos_peer(k))))
                def third(k=k, i=i):
                    lat_copy(k, i).start()

        for k in range(1, group):
            q_copy(k, i).start()
        if i > 0:
            for k in cross:

                @pl.when(near(pos_peer(k)))
                def fourth(k=k, i=i):
                    lat_copy(k, i).start()

            for k in inner:
                lat_copy(k, i).start()

    rows_dev = q_buf.shape[2]
    width = q_buf.shape[3]
    rows_all = group * rows_dev
    lat_dev = lat_buf.shape[2]
    lat_width = lat_buf.shape[3]
    head_dim = width // HEADS
    power_scale = float(head_dim) ** (-0.5) * math.log2(math.e)
    vocab = w_vocab.shape[0]

    for copy in local:
        copy.wait()
    for raw, turned in (
        (w_query, w_query_t),
        (w_out, w_out_t),
        (w_up, w_up_t),
        (w_down, w_down_t),
    ):
        turned[...] = raw[...].T
    gain_col[...] = jnp.broadcast_to(mlp_gain[...].reshape(1, width), (LANES, width)).T
    turn_buf[...] = jnp.zeros_like(turn_buf)
    bias_row[...] = jnp.zeros_like(bias_row)
    bias_row[:, :vocab] = vocab_bias[...].reshape(1, vocab)
    bias_col[...] = jnp.broadcast_to(bias_row[...], (LANES, bias_row.shape[1])).T

    def wide(column):
        return jnp.concatenate([column] * (rows_all // LANES), axis=1)

    for k in range(1, group):
        t_copy(k).wait_recv()
        m_copy(k).wait_recv()

    def prepare(i):
        for k in range(1, group):
            q_copy(k, i).wait_recv()
        turned = q_buf[:, i].reshape(rows_all, width).T
        x_t[i] = turned.astype(jnp.float32)
        query_t = dot(w_query_t[...], turned).astype(jnp.bfloat16)
        for h in range(HEADS):
            low, high, begin, end = head_span(h, head_dim)
            if low > begin:
                q_pad[i, h, : low - begin] = jnp.zeros((low - begin, rows_all), jnp.bfloat16)
            q_pad[i, h, low - begin : high - begin] = query_t[low:high]
            if end > high:
                q_pad[i, h, high - begin : end - begin] = jnp.zeros(
                    (end - high, rows_all), jnp.bfloat16
                )

    acc[...] = jnp.zeros_like(acc)

    slots = n_pos // LAT_SPLIT
    lat_rows = slots * lat_dev
    some = max(1, min(slots, 64 // lat_dev))
    chunk = 256

    def hand_over(i):
        logit_buf[i] = (
            turn_buf[i].T[:, :vocab].astype(jnp.bfloat16).reshape(group, rows_dev, vocab)
        )
        for k in range(1, group):
            out_copy(k, i).start()
        out_local(i).start()

    def one_sequence(i, carry):
        prepare(i)

        @pl.when(i > 0)
        def earlier():
            hand_over(i - 1)

        for part in reversed(range(LAT_SPLIT)):
            base_row = part * lat_rows
            for start in range(part * slots, (part + 1) * slots, some):
                for k in range(start, start + some):
                    if k == 0:
                        lat_local(i).wait()
                    else:
                        lat_copy(k, i).wait_recv()
                field = lat_buf[i, start : start + some].astype(jnp.float32)
                field = field.reshape(some * lat_dev, lat_width)
                norm_buf[start * lat_dev : (start + some) * lat_dev] = layer_norm(
                    field, kv_gain[...].reshape(1, lat_width), 1
                ).astype(jnp.bfloat16)
            normed_lat = norm_buf[base_row : base_row + lat_rows]
            for start in range(0, 2 * width, chunk):
                block_kv = dot(normed_lat, w_kv[:, start : start + chunk]).astype(jnp.bfloat16)
                if start < width:
                    k_buf[base_row : base_row + lat_rows, start : start + chunk] = block_kv
                else:
                    v_t[start - width : start - width + chunk, base_row : base_row + lat_rows] = (
                        block_kv.T
                    )

        for h in range(HEADS):
            low, high, begin, end = head_span(h, head_dim)
            scores = dot(k_buf[:, begin:end], q_pad[i, h, : end - begin])
            score_buf[h] = scores
            top_buf[h : h + 1] = jnp.max(scores, axis=0, keepdims=True)
        for h in range(HEADS):
            power = jnp.exp2((score_buf[h] - top_buf[h : h + 1]) * power_scale)
            total_buf[h : h + 1] = jnp.sum(power, axis=0, keepdims=True)
            power_buf[h] = power.astype(jnp.bfloat16)
        for h in range(HEADS):
            low, high = h * head_dim, (h + 1) * head_dim
            mixed = dot(v_t[low:high], power_buf[h])
            att_t[low:high] = (mixed * (1.0 / total_buf[h : h + 1])).astype(jnp.bfloat16)

        half = width // 2
        first = x_t[i] + dot_parts(w_out_t, att_t[...], half)
        normed = layer_norm(first, wide(gain_col[...]), 0).astype(jnp.bfloat16)
        hidden = jax.nn.gelu(dot_parts(w_up_t, normed, half)).astype(jnp.bfloat16)
        output = (first + dot_parts(w_down_t, hidden, half)).astype(jnp.bfloat16)
        full_logits = dot_parts(w_vocab, output, LANES) + wide(bias_col[:vocab])
        turn_buf[i, :vocab] = full_logits
        line = mine * seqs + i
        target = jnp.concatenate([t_buf[k, pl.ds(line, 1)] for k in range(group)], axis=1)
        weight = jnp.concatenate([m_buf[k, pl.ds(line, 1)] for k in range(group)], axis=1)
        weight = weight.astype(jnp.float32)
        ids = lax.broadcasted_iota(jnp.int32, full_logits.shape, 0)
        picked = jnp.sum(jnp.where(ids == target, full_logits, 0.0), axis=0, keepdims=True)
        top = jnp.max(full_logits, axis=0, keepdims=True)
        spread = jnp.log(jnp.sum(jnp.exp(full_logits - top), axis=0, keepdims=True))
        cross_loss = (top + spread - picked) * weight
        for start in range(0, rows_all, LANES):
            acc[:, :LANES] += cross_loss[:, start : start + LANES]
            acc[:, LANES:] += weight[:, start : start + LANES]

        return carry

    lax.fori_loop(0, seqs, one_sequence, 0)

    n_all = n_pos * n_head
    rank = me * n_head + my_head

    swaps = [k // 2 if k % 2 == 0 else n_all - 1 - k // 2 for k in range(n_all)]

    def p_peer(k):
        return lax.rem(2 * n_all - 1 - rank + k, n_all)

    def p_each(act):
        for k in swaps:

            @pl.when(p_peer(k) != rank)
            def other(k=k):
                act(p_copy(k))

    def p_copy(k):
        peer = p_peer(k)
        return pltpu.make_async_remote_copy(
            src_ref=part_src,
            dst_ref=part_all.at[rank],
            send_sem=p_send.at[k],
            recv_sem=p_recv.at[k],
            device_id={"pos": peer // n_head, "head": lax.rem(peer, n_head)},
            device_id_type=MESH,
        )

    part = acc[...]
    part_src[...] = part
    part_all[rank] = part
    p_each(lambda copy: copy.start())
    hand_over(seqs - 1)
    p_each(lambda copy: copy.wait_recv())
    whole = jnp.sum(part_all[...], axis=0)
    mean = jnp.sum(whole[:, :LANES], axis=1, keepdims=True) / jnp.sum(
        whole[:, LANES:], axis=1, keepdims=True
    )
    loss_out[...] = jnp.broadcast_to(mean, loss_out.shape)

    p_each(lambda copy: copy.wait_send())
    for k in range(1, group):
        for i in range(seqs):
            q_copy(k, i).wait_send()
        t_copy(k).wait_send()
        m_copy(k).wait_send()
    for i in range(seqs):
        for k in range(1, n_pos):
            lat_copy(k, i).wait_send()
        out_local(i).wait()
        for k in range(1, group):
            out_copy(k, i).wait()


def deliver(logits, loss, logits_out, loss_out, sems):
    copy = pltpu.make_async_copy(logits, logits_out, sems.at[0])
    copy.start()
    loss_out[...] = loss[0:1, 0:1]
    copy.wait()


def on_device(n_pos, n_head, *args):
    (queries, latents, w_query, kv_gain, w_kv, w_out, mlp_gain, w_up, w_down, w_vocab, vocab_bias, targets, mask) = args
    batch_dev, pos_dev, width = queries.shape
    lat_dev, lat_width = latents.shape[1:]
    vocab = w_vocab.shape[1]
    group = max(1, min(n_pos, batch_dev) // 2)
    seqs = batch_dev // group
    assert n_pos % group == 0 and batch_dev % group == 0
    rows_all = group * pos_dev
    assert rows_all % LANES == 0 and n_pos % LAT_SPLIT == 0
    vocab_pad = -(-vocab // LANES) * LANES
    hbm = pl.BlockSpec(memory_space=pltpu.HBM)
    vmem = pl.BlockSpec(memory_space=pltpu.VMEM)
    dma = pltpu.SemaphoreType.DMA
    bf16, f32 = jnp.bfloat16, jnp.float32
    logits, loss = pl.pallas_call(
        functools.partial(kernel, n_pos, n_head, group, seqs),
        out_shape=(
            pltpu.VMEM((batch_dev, pos_dev, vocab), bf16),
            pltpu.VMEM((8, LANES), f32),
        ),
        in_specs=[hbm, hbm, hbm, vmem, hbm, hbm, vmem, hbm, hbm, hbm, vmem, hbm, hbm],
        out_specs=(vmem, vmem),
        scratch_shapes=[
            pltpu.VMEM(latents.shape, bf16),
            pltpu.VMEM(queries.shape, bf16),
            pltpu.VMEM((seqs, n_pos, lat_dev, lat_width), bf16),
            pltpu.VMEM((group, seqs, pos_dev, width), bf16),
            pltpu.VMEM((group, batch_dev, pos_dev), jnp.int32),
            pltpu.VMEM((group, batch_dev, pos_dev), jnp.int32),
            pltpu.VMEM(w_query.shape, bf16),
            pltpu.VMEM(w_kv.shape, bf16),
            pltpu.VMEM(w_out.shape, bf16),
            pltpu.VMEM(w_up.shape, bf16),
            pltpu.VMEM(w_down.shape, bf16),
            pltpu.VMEM(w_vocab.shape[::-1], bf16),
            pltpu.VMEM(w_query.shape[::-1], bf16),
            pltpu.VMEM(w_out.shape[::-1], bf16),
            pltpu.VMEM(w_up.shape[::-1], bf16),
            pltpu.VMEM(w_down.shape[::-1], bf16),
            pltpu.VMEM((width, LANES), f32),
            pltpu.VMEM((1, vocab_pad), f32),
            pltpu.VMEM((vocab_pad, LANES), f32),
            pltpu.VMEM((seqs, width, rows_all), f32),
            pltpu.VMEM((seqs, HEADS, 2 * LANES, rows_all), bf16),
            pltpu.VMEM((n_pos * lat_dev, lat_width), bf16),
            pltpu.VMEM((n_pos * lat_dev, width), bf16),
            pltpu.VMEM((width, n_pos * lat_dev), bf16),
            pltpu.VMEM((HEADS, n_pos * lat_dev, rows_all), f32),
            pltpu.VMEM((HEADS, rows_all), f32),
            pltpu.VMEM((HEADS, rows_all), f32),
            pltpu.VMEM((HEADS, n_pos * lat_dev, rows_all), bf16),
            pltpu.VMEM((width, rows_all), bf16),
            pltpu.VMEM((seqs, vocab_pad, rows_all), f32),
            pltpu.VMEM((seqs, group, pos_dev, vocab), bf16),
            pltpu.VMEM((1, 2 * LANES), f32),
            pltpu.VMEM((1, 2 * LANES), f32),
            pltpu.VMEM((n_pos * n_head, 1, 2 * LANES), f32),
            dma((seqs, n_pos)),
            dma((seqs, n_pos)),
            pltpu.SemaphoreType.DMA,
            dma((seqs, group)),
            dma((seqs, group)),
            dma((group,)),
            dma((group,)),
            dma((group,)),
            dma((group,)),
            dma((seqs, group)),
            dma((seqs, group)),
            dma((n_pos * n_head,)),
            dma((n_pos * n_head,)),
            dma((6,)),
            dma((2,)),
            pltpu.SemaphoreType.REGULAR((2,)),
        ],
        compiler_params=pltpu.CompilerParams(
            collective_id=0, has_side_effects=True, vmem_limit_bytes=60 * 1024 * 1024
        ),
    )(
        queries,
        latents,
        w_query,
        kv_gain,
        w_kv,
        w_out,
        mlp_gain,
        w_up,
        w_down,
        w_vocab.T,
        vocab_bias,
        targets,
        mask,
    )
    logits, loss = pl.pallas_call(
        deliver,
        out_shape=(
            jax.ShapeDtypeStruct((batch_dev, pos_dev, vocab), bf16),
            jax.ShapeDtypeStruct((1, 1), f32),
        ),
        in_specs=[pl.BlockSpec(memory_space=pl.ANY), vmem],
        out_specs=(hbm, vmem),
        scratch_shapes=[pltpu.SemaphoreType.DMA((2,))],
        compiler_params=pltpu.CompilerParams(vmem_limit_bytes=1024 * 1024),
    )(logits, loss)
    return (logits, loss.reshape(()))


def solution(mesh):
    in_specs = (
        P("head", "pos", None),
        P("head", "pos", None),
        P(),
        P(),
        P(),
        P(),
        P(),
        P(),
        P(),
        P(),
        P(),
        P("head", "pos"),
        P("head", "pos"),
    )
    out_specs = (P("head", "pos", None), P())
    return jax.shard_map(
        functools.partial(on_device, mesh.shape["pos"], mesh.shape["head"]),
        mesh=mesh,
        in_specs=in_specs,
        out_specs=out_specs,
        check_vma=False,
    )
```
